32 devices in a mesh: orb: 8 (over y, x, core), walk: 4 (over z).
Axes of the slice: x: 2, y: 2, z: 4, core: 2. Of those that a mesh axis runs over, the one named last changes fastest.
Arguments:
- chol: bfloat16 [32, 2048, 2048], P(None, 'orb', 'walk'), may hold values from -6 to 6
- orbitals: bfloat16 [2048, 1024], replicated, may hold values from -0.125 to 0.125
- greens: bfloat16 [4, 1024, 2048], P('walk'), may hold values from -0.00390625 to 0.00390625
- shift: float32 [32], P('orb'), may hold values from -6 to 6
Outputs:
- force_bias: float32 [4, 32], P('walk', 'orb')
- rotated: bfloat16 [32, 1024, 2048], P('orb', None, 'walk')
The draws below stay inside these ranges and needn't reach their ends.
All inputs are finite; a program needn't handle non-finite values.
Results may differ from the reference program's by a relative error of at most 0.007.
Values may be sent and summed in bfloat16 or wider, within the bound.
No kernel may reach another device: no remote copies, remote signals or barrier semaphores. Data moves between devices by JAX's collectives and lax.ppermute only.
A program may use at most 64 MiB of HBM per device.

```python
import jax
import jax.numpy as jnp
from jax import lax

N = 2048
NOCC = 1024
NV = 32
W = 4


def shard_levels(stream_key, shape, pieces, smallest, top_value):
    def one(dim, parts):
        heights = jax.random.uniform(jax.random.fold_in(jax.random.fold_in(stream_key, 6), dim), (parts,), jnp.float32, smallest / len(pieces), top_value / len(pieces))
        return jnp.repeat(jnp.exp(heights), shape[dim] // parts).reshape((-1,) + (1,) * (len(shape) - dim - 1))

    factor_of = one(*pieces[0])
    for cut in pieces[1:]:
        factor_of = factor_of * one(*cut)
    return factor_of


def normal_values(own_key, shape, width, limit, split=(), kind=jnp.bfloat16):
    loudness = shard_levels(own_key, shape, split, -0.22, 0.18) if split else 1.0
    result = jax.random.normal(own_key, shape, jnp.float32) * width * loudness
    return jnp.minimum(jnp.maximum(result, -limit), limit).astype(kind)


def setup_inputs(seed: int = 0) -> dict:
    key_list = jax.random.split(jax.random.key(seed), 5)
    chol = normal_values(key_list[0], (NV, N, N), 1.0, 6.0, ((1, 8), (2, 4)))
    orbitals = normal_values(key_list[1], (N, NOCC), N ** -0.5, 0.125)
    greens = normal_values(key_list[2], (W, NOCC, N), (NOCC * N) ** -0.5, 0.00390625, ((0, 4),))
    shift = normal_values(key_list[3], (NV,), 1.0, 6.0, ((0, 8),), jnp.float32)
    return dict(chol=chol, orbitals=orbitals, greens=greens, shift=shift)


def reference(chol, orbitals, greens, shift):
    flat_greens = greens.reshape(greens.shape[0], -1).astype(jnp.float32)
    orbitals_t = orbitals.T

    def one_vector(matrix):
        rotation = jnp.dot(orbitals_t, matrix, preferred_element_type=jnp.float32)
        column = jnp.dot(flat_greens, rotation.reshape(-1), precision=lax.Precision.HIGHEST)
        return rotation.astype(jnp.bfloat16), column

    rotated, columns = lax.map(one_vector, chol)
    force_bias = columns.T - shift[None, :]
    return (force_bias, rotated)
```

```python
import functools

import jax
import jax.numpy as jnp
from jax import lax
from jax.experimental import pallas as pl
from jax.experimental.pallas import tpu as pltpu
from jax.sharding import PartitionSpec as P

MIB = 2**20


def tied(value, *after):
    return lax.optimization_barrier((value, *after))[0]


def params(mib):
    return pltpu.CompilerParams(vmem_limit_bytes=mib * MIB)


def cost(flops, moved):
    return pl.CostEstimate(flops=flops, bytes_accessed=moved, transcendentals=0)


def terms_kernel(place, chol_ref, *refs):
    product_refs, out_ref = refs[:-1], refs[-1]
    block = chol_ref[0].astype(jnp.float32)
    for w, product in enumerate(product_refs):
        out_ref[w, 0] = jnp.sum(product[...].astype(jnp.float32) * block, axis=0, keepdims=True)


def force_terms(chol, products, me, count):
    vectors, rows, columns = chol.shape
    walkers = len(products)
    whole = pl.BlockSpec((rows, columns), lambda v, place: (0, 0))
    return pl.pallas_call(
        terms_kernel,
        out_shape=jax.ShapeDtypeStruct((walkers, vectors, 1, columns), jnp.float32),
        grid_spec=pltpu.PrefetchScalarGridSpec(
            num_scalar_prefetch=1,
            grid=(vectors,),
            in_specs=[
                pl.BlockSpec(
                    (1, rows, columns),
                    lambda v, place: ((place[0] ^ (v // count)) * count + v % count, 0, 0),
                )
            ]
            + [whole] * walkers,
            out_specs=pl.BlockSpec((walkers, 1, 1, columns), lambda v, place: (0, v, 0, 0)),
        ),
        compiler_params=params(16),
        cost_estimate=cost(2 * walkers * chol.size, 2 * chol.size),
        name="terms",
    )(me, chol, *products)


def near_kernel(place, lhs_ref, *refs):
    block_refs, out_ref, rhs = refs[:-2], refs[-2], refs[-1]
    rows = block_refs[0].shape[1]
    for k, block in enumerate(block_refs):
        rhs[k * rows : (k + 1) * rows, :] = block[0]
    out_ref[0] = jnp.dot(lhs_ref[...], rhs[...], preferred_element_type=jnp.float32)


def near_sum(lhs, chol, blocks, me):
    count, rows, columns = blocks[0].shape
    occupied, depth = lhs.shape
    tile = occupied // 2
    return pl.pallas_call(
        near_kernel,
        out_shape=jax.ShapeDtypeStruct((count, occupied, columns), jnp.float32),
        grid_spec=pltpu.PrefetchScalarGridSpec(
            num_scalar_prefetch=1,
            grid=(count, occupied // tile),
            in_specs=[
                pl.BlockSpec((tile, depth), lambda g, i, place: (i, 0)),
                pl.BlockSpec((1, rows, columns), lambda g, i, place: (place[0] * count + g, 0, 0)),
            ]
            + [pl.BlockSpec((1, rows, columns), lambda g, i, place: (g, 0, 0))] * len(blocks),
            out_specs=pl.BlockSpec((1, tile, columns), lambda g, i, place: (g, i, 0)),
            scratch_shapes=[pltpu.VMEM((depth, columns), jnp.bfloat16)],
        ),
        compiler_params=params(24),
        cost_estimate=cost(2 * count * occupied * depth * columns, 4 * count * occupied * columns),
        name="near",
    )(me, lhs, chol, *blocks)


def far_kernel(lhs_ref, near_ref, *refs):
    out_ref, rhs = refs[-2:]
    block_refs = [r for r in refs[:-2] if len(r.shape) == 3 and r.shape[0] == 1]
    rows = block_refs[0].shape[1]
    for k, block in enumerate(block_refs):
        rhs[k * rows : (k + 1) * rows, :] = block[0]
    total = near_ref[0] + jnp.dot(lhs_ref[...], rhs[...], preferred_element_type=jnp.float32)
    out_ref[0] = total.astype(out_ref.dtype)


def far_sum(lhs, near, blocks, rotated, g):
    _, rows, columns = blocks[0].shape
    occupied, depth = lhs.shape
    tile = occupied // 4
    return pl.pallas_call(
        far_kernel,
        out_shape=jax.ShapeDtypeStruct(near.shape, jnp.bfloat16),
        grid=(occupied // tile,),
        in_specs=[
            pl.BlockSpec((tile, depth), lambda i: (i, 0)),
            pl.BlockSpec((1, tile, columns), lambda i: (g, i, 0)),
        ]
        + [pl.BlockSpec((1, rows, columns), lambda i: (0, 0, 0))] * len(blocks)
        + [pl.BlockSpec(memory_space=pl.ANY)] * (rotated is not None),
        out_specs=pl.BlockSpec((1, tile, columns), lambda i: (g, i, 0)),
        scratch_shapes=[pltpu.VMEM((depth, columns), jnp.bfloat16)],
        input_output_aliases={2 + len(blocks): 0} if rotated is not None else {},
        compiler_params=params(12),
        cost_estimate=cost(2 * occupied * depth * columns, 4 * occupied * columns),
        name="far",
    )(lhs, near, *blocks, *([] if rotated is None else [rotated]))


def local(owners, chol, orbitals, greens, shift):
    walkers = chol.shape[2] and greens.shape[2] // chol.shape[2]
    count = chol.shape[0] // owners
    rows, columns = chol.shape[1:]
    me, mine = lax.axis_index("orb"), lax.axis_index("walk")
    chips = lambda k: (k >> 1).bit_count()
    offsets = sorted(range(1, owners), key=lambda k: (chips(k), k & 1, k))
    near_offsets = [k for k in offsets if chips(k) <= 1]
    far_offsets = [k for k in offsets if chips(k) > 1]

    def swap(value, axis, k, size):
        return lax.ppermute(value, axis, [(i, i ^ k) for i in range(size)])

    def part(source, k, start, size):
        return lax.dynamic_slice_in_dim(source, (me ^ k) * count + start, size, 0)

    near = {}
    source = chol
    for k in near_offsets:
        piece = part(source, k, 0, count)
        near[k] = swap(piece, "orb", k, owners)

    orbital_rows = lax.dynamic_slice_in_dim(orbitals, me * rows, rows, 0)
    products = jnp.dot(orbital_rows, greens[0], preferred_element_type=jnp.float32)
    products = products.astype(jnp.bfloat16)
    arrived = []
    for k in range(walkers):
        piece = lax.dynamic_slice_in_dim(products, (mine ^ k) * columns, columns, 1)
        arrived.append(swap(piece, "walk", k, walkers) if k else piece)
    place = jnp.stack([me, mine]).astype(jnp.int32)
    terms = force_terms(chol, arrived, place, count)
    terms = terms.sum(axis=(2, 3))

    total = terms[0]
    for k in range(1, walkers):
        total = total + swap(terms[k], "walk", k, walkers)
    total = total.reshape(owners, count)
    span = owners
    while span > 1:
        span //= 2
        total = total[:span] + swap(total[span:], "orb", span, owners)
    force_bias = total - shift[None, :]

    order = [0] + near_offsets + far_offsets
    lhs = jnp.concatenate(
        [lax.dynamic_slice_in_dim(orbitals, (me ^ k) * rows, rows, 0) for k in order], 0
    ).T
    depth = rows * (1 + len(near_offsets))
    partial = near_sum(lhs[:, :depth], chol, [near[k] for k in near_offsets], place)
    lhs_far = lhs[:, depth:]
    rotated = None
    for g in range(count):
        blocks = [swap(part(source, k, g, 1), "orb", k, owners) for k in far_offsets]
        rotated = far_sum(lhs_far, partial, blocks, rotated, g)
    return force_bias, rotated


def solution(mesh):
    in_specs = (P(None, "orb", "walk"), P(), P("walk", None, None), P("orb"))
    out_specs = (P("walk", "orb"), P("orb", None, "walk"))
    body = functools.partial(local, mesh.shape["orb"])
    return jax.shard_map(body, mesh=mesh, in_specs=in_specs, out_specs=out_specs, check_vma=False)
```

```python
import functools

import jax
import jax.numpy as jnp
from jax import lax
from jax.experimental import pallas as pl
from jax.experimental.pallas import tpu as pltpu
from jax.sharding import PartitionSpec as P


MIB = 2**20


def tied(value, *after):
    return lax.optimization_barrier((value, *after))[0]


def params(mib):
    return pltpu.CompilerParams(vmem_limit_bytes=mib * MIB)


def chips(k):
    return (k >> 1).bit_count()


def cost(flops, moved):
    return pl.CostEstimate(flops=flops, bytes_accessed=moved, transcendentals=0)


def terms_kernel(place, chol_ref, *refs):
    product_refs, out_ref = refs[:-1], refs[-1]
    block = chol_ref[0].astype(jnp.float32)
    for w, product in enumerate(product_refs):
        out_ref[w, 0] = jnp.sum(product[...].astype(jnp.float32) * block, axis=0, keepdims=True)


def force_terms(chol, products, me, count):
    vectors, rows, columns = chol.shape
    walkers = len(products)
    whole = pl.BlockSpec((rows, columns), lambda v, place: (0, 0))
    return pl.pallas_call(
        terms_kernel,
        out_shape=jax.ShapeDtypeStruct((walkers, vectors, 1, columns), jnp.float32),
        grid_spec=pltpu.PrefetchScalarGridSpec(
            num_scalar_prefetch=1,
            grid=(vectors,),
            in_specs=[
                pl.BlockSpec(
                    (1, rows, columns),
                    lambda v, place: ((place[0] ^ (v // count)) * count + v % count, 0, 0),
                )
            ]
            + [whole] * walkers,
            out_specs=pl.BlockSpec((walkers, 1, 1, columns), lambda v, place: (0, v, 0, 0)),
        ),
        compiler_params=params(56),
        cost_estimate=cost(2 * walkers * chol.size, 2 * chol.size),
        name="terms",
    )(me, chol, *products)


def turn_kernel(place, source_ref, out_ref):
    out_ref[...] = source_ref[...].T


def turned(orbitals, owners, rows):
    occupied = orbitals.shape[1]
    blocks = owners.shape[0]
    return pl.pallas_call(
        turn_kernel,
        out_shape=jax.ShapeDtypeStruct((occupied, blocks * rows), orbitals.dtype),
        grid_spec=pltpu.PrefetchScalarGridSpec(
            num_scalar_prefetch=1,
            grid=(blocks,),
            in_specs=[pl.BlockSpec((rows, occupied), lambda k, place: (place[k], 0))],
            out_specs=pl.BlockSpec((occupied, rows), lambda k, place: (0, k)),
        ),
        compiler_params=params(8),
        cost_estimate=cost(blocks * rows * occupied * 300, 4 * blocks * rows * occupied),
        name="turn",
    )(owners, orbitals)


def near_kernel(lhs_ref, *refs):
    block_refs, out_ref, rhs = refs[:-2], refs[-2], refs[-1]
    rows = block_refs[0].shape[1]
    for k, block in enumerate(block_refs):
        rhs[k * rows : (k + 1) * rows, :] = block[0]
    out_ref[0] = jnp.dot(lhs_ref[...], rhs[...], preferred_element_type=jnp.float32)


def near_sum(lhs, blocks):
    count, rows, columns = blocks[0].shape
    occupied, depth = lhs.shape
    return pl.pallas_call(
        near_kernel,
        out_shape=jax.ShapeDtypeStruct((count, occupied, columns), jnp.float32),
        grid=(count,),
        in_specs=[pl.BlockSpec((occupied, depth), lambda g: (0, 0))]
        + [pl.BlockSpec((1, rows, columns), lambda g: (g, 0, 0))] * len(blocks),
        out_specs=pl.BlockSpec((1, occupied, columns), lambda g: (g, 0, 0)),
        scratch_shapes=[pltpu.VMEM((depth, columns), jnp.bfloat16)],
        compiler_params=params(24),
        cost_estimate=cost(2 * count * occupied * depth * columns, 4 * count * occupied * columns),
        name="near",
    )(lhs, *blocks)


def far_kernel(g, blocks, lhs_ref, near_ref, *refs):
    block_refs, (out_ref, rhs, held, sems) = refs[:blocks], refs[-4:]
    rows = block_refs[0].shape[1]
    for k, block in enumerate(block_refs):
        rhs[k * rows : (k + 1) * rows, :] = block[0]
    tiles = sems.shape[0]
    tile = held.shape[0] // tiles
    copies = []
    for t in range(tiles):
        part = pl.ds(t * tile, tile)
        total = near_ref[g, part, :] + jnp.dot(
            lhs_ref[part, :], rhs[...], preferred_element_type=jnp.float32
        )
        held[part, :] = total.astype(held.dtype)
        copy = pltpu.make_async_copy(held.at[part, :], out_ref.at[g, part, :], sems.at[t])
        copy.start()
        copies.append(copy)
    for copy in copies:
        copy.wait()


def far_sum(lhs, near, blocks, rotated, g):
    _, _, columns = blocks[0].shape
    occupied, depth = lhs.shape
    tiles = 4
    held = [] if rotated is None else [rotated]
    whole, left = pl.BlockSpec(memory_space=pltpu.VMEM), pl.BlockSpec(memory_space=pl.ANY)
    return pl.pallas_call(
        functools.partial(far_kernel, g, len(blocks)),
        out_shape=jax.ShapeDtypeStruct(near.shape, jnp.bfloat16),
        in_specs=[whole] * (2 + len(blocks)) + [left] * len(held),
        out_specs=left,
        scratch_shapes=[
            pltpu.VMEM((depth, columns), jnp.bfloat16),
            pltpu.VMEM((occupied, columns), jnp.bfloat16),
            pltpu.SemaphoreType.DMA((tiles,)),
        ],
        input_output_aliases={2 + len(blocks): 0} if held else {},
        compiler_params=params(16),
        cost_estimate=cost(2 * occupied * depth * columns, 4 * occupied * columns),
        name="far",
    )(lhs, near, *blocks, *held)


def local(owners, chol, orbitals, greens, shift):
    walkers = greens.shape[2] // chol.shape[2]
    count = chol.shape[0] // owners
    rows, columns = chol.shape[1:]
    me, mine = lax.axis_index("orb"), lax.axis_index("walk")
    near_offsets = sorted((k for k in range(1, owners) if chips(k) <= 1), key=lambda k: (chips(k) != 1, k & 1, k))
    far_offsets = [k for k in range(1, owners) if chips(k) > 1]
    first = [k for k in near_offsets if chips(k) and not k & 1]

    def swap(value, axis, k, size):
        return lax.ppermute(value, axis, [(i, i ^ k) for i in range(size)])

    def part(source, k, start=0, size=count):
        return lax.dynamic_slice_in_dim(source, (me ^ k) * count + start, size, 0)

    near = {}
    pieces = [part(chol, k) for k in first]
    for k, piece in zip(first, pieces):
        near[k] = swap(piece, "orb", k, owners)

    orbitals, greens, chol_next = tied((orbitals, greens, chol), *pieces)
    orbital_rows = lax.dynamic_slice_in_dim(orbitals, me * rows, rows, 0)
    products = jnp.dot(orbital_rows, greens[0], preferred_element_type=jnp.float32)
    products = products.astype(jnp.bfloat16)
    arrived = []
    for k in range(walkers):
        piece = lax.dynamic_slice_in_dim(products, (mine ^ k) * columns, columns, 1)
        arrived.append(swap(piece, "walk", k, walkers) if k else piece)

    chol_next = tied(chol_next, products)
    near[0] = part(chol_next, 0)
    pieces = {k: part(chol_next, k) for k in near_offsets if k not in near}
    for k, piece in pieces.items():
        near[k] = swap(piece, "orb", k, owners)
    far = {}
    chol_next = tied(chol_next, *pieces.values())
    for k in far_offsets:
        far[0, k] = swap(part(chol_next, k, 0, 1), "orb", k, owners)

    order = jnp.array([0] + near_offsets, jnp.int32) ^ me
    lhs_near = turned(orbitals, order, rows)
    lhs_far = turned(orbitals, jnp.array(far_offsets, jnp.int32) ^ me, rows)

    terms = force_terms(chol, arrived, jnp.stack([me, mine]).astype(jnp.int32), count)
    terms = terms.sum(axis=(2, 3))
    total = terms[0] + sum(swap(terms[k], "walk", k, walkers) for k in range(1, walkers))
    total = total.reshape(owners, count)
    even, odd = total[0::2], total[1::2]
    even = even + swap(odd, "orb", 1, owners)
    arrivals = [swap(even[k : k + 1], "orb", 2 * k, owners) for k in range(1, owners // 2)]

    chol_next = tied(chol_next, even)
    for g in range(1, count):
        for k in far_offsets:
            far[g, k] = swap(part(chol_next, k, g, 1), "orb", k, owners)

    partial = near_sum(lhs_near, [near[k] for k in [0] + near_offsets])
    arrivals = tied(arrivals, partial)
    force_bias = even[:1] + sum(arrivals) - shift[None, :]
    rotated = None
    for g in range(count):
        rotated = far_sum(lhs_far, partial, [far[g, k] for k in far_offsets], rotated, g)
    return force_bias, rotated


def solution(mesh):
    in_specs = (P(None, "orb", "walk"), P(), P("walk", None, None), P("orb"))
    out_specs = (P("walk", "orb"), P("orb", None, "walk"))
    owners = mesh.shape["orb"]

    def body(*args):
        return local(owners, *args)

    return jax.shard_map(body, mesh=mesh, in_specs=in_specs, out_specs=out_specs, check_vma=False)
```

```python
import functools

import jax
import jax.numpy as jnp
from jax import lax
from jax.experimental import pallas as pl
from jax.experimental.pallas import tpu as pltpu
from jax.sharding import PartitionSpec as P


MIB = 2**20


def tied(value, *after):
    return lax.optimization_barrier((value, *after))[0]


def params(mib):
    return pltpu.CompilerParams(vmem_limit_bytes=mib * MIB)


def offsets(owners):
    chips = lambda k: (k >> 1).bit_count()
    first = [k for k in range(owners - 2, 0, -2) if chips(k) == 1]
    second = [k + 1 for k in first] + [1]
    return first, second, [k for k in range(1, owners) if chips(k) > 1]


def cost(flops, moved):
    return pl.CostEstimate(flops=flops, bytes_accessed=moved, transcendentals=0)


def terms_kernel(place, chol_ref, *refs):
    product_refs, out_ref = refs[:-1], refs[-1]
    for v in range(chol_ref.shape[0]):
        block = chol_ref[v].astype(jnp.float32)
        for w, product in enumerate(product_refs):
            terms = jnp.sum(product[...].astype(jnp.float32) * block, axis=0, keepdims=True)
            out_ref[w, v] = terms


def force_terms(chol, products, me, count):
    vectors, rows, columns = chol.shape
    walkers = len(products)
    whole = pl.BlockSpec((rows, columns), lambda v, place: (0, 0))
    return pl.pallas_call(
        terms_kernel,
        out_shape=jax.ShapeDtypeStruct((walkers, vectors, 1, columns), jnp.float32),
        grid_spec=pltpu.PrefetchScalarGridSpec(
            num_scalar_prefetch=1,
            grid=(vectors // count,),
            in_specs=[pl.BlockSpec((count, rows, columns), lambda v, place: (place[0] ^ v, 0, 0))]
            + [whole] * walkers,
            out_specs=pl.BlockSpec((walkers, count, 1, columns), lambda v, place: (0, v, 0, 0)),
        ),
        compiler_params=params(56),
        cost_estimate=cost(2 * walkers * chol.size, 2 * chol.size),
        name="terms",
    )(me, chol, *products)


def turn_kernel(place, source_ref, out_ref):
    out_ref[...] = source_ref[...].T


def turned(orbitals, owners, rows):
    occupied = orbitals.shape[1]
    blocks = owners.shape[0]
    return pl.pallas_call(
        turn_kernel,
        out_shape=jax.ShapeDtypeStruct((occupied, blocks * rows), orbitals.dtype),
        grid_spec=pltpu.PrefetchScalarGridSpec(
            num_scalar_prefetch=1,
            grid=(blocks,),
            in_specs=[pl.BlockSpec((rows, occupied), lambda k, place: (place[k], 0))],
            out_specs=pl.BlockSpec((occupied, rows), lambda k, place: (0, k)),
        ),
        compiler_params=params(8),
        cost_estimate=cost(blocks * rows * occupied * 300, 4 * blocks * rows * occupied),
        name="turn",
    )(owners, orbitals)


def near_kernel(counts, lhs_ref, *refs):
    piece_refs, out_ref, rhs = refs[:-2], refs[-2], refs[-1]
    rows = piece_refs[0].shape[1]
    vector = pl.program_id(0)
    piece_refs = iter(piece_refs)
    for k, pieces in enumerate(counts):
        at, start = pl.ds(k * rows, rows), 0
        for size in pieces:
            piece = next(piece_refs)

            @pl.when((vector >= start) & (vector < start + size))
            def _():
                rhs[at, :] = piece[0]

            start += size
    out_ref[0] = jnp.dot(lhs_ref[...], rhs[...], preferred_element_type=jnp.float32)


def near_sum(lhs, blocks):
    counts = [[piece.shape[0] for piece in pieces] for pieces in blocks]
    count, (_, rows, columns) = sum(counts[0]), blocks[0][0].shape
    occupied, depth = lhs.shape
    specs = [pl.BlockSpec((occupied, depth), lambda g: (0, 0))]
    for pieces in counts:
        start = 0
        for size in pieces:
            at = functools.partial(lambda start, size, g: (jnp.clip(g - start, 0, size - 1), 0, 0), start, size)
            specs.append(pl.BlockSpec((1, rows, columns), at))
            start += size
    return pl.pallas_call(
        functools.partial(near_kernel, counts),
        out_shape=jax.ShapeDtypeStruct((count, occupied, columns), jnp.float32),
        grid=(count,),
        in_specs=specs,
        out_specs=pl.BlockSpec((1, occupied, columns), lambda g: (g, 0, 0)),
        scratch_shapes=[pltpu.VMEM((depth, columns), jnp.bfloat16)],
        compiler_params=params(24),
        cost_estimate=cost(2 * count * occupied * depth * columns, 4 * count * occupied * columns),
        name="near",
    )(lhs, *(piece for pieces in blocks for piece in pieces))


def far_kernel(first, blocks, lhs_ref, near_ref, *refs):
    block_refs, (out_ref, rhs, held, sems) = refs[:blocks], refs[-4:]
    size, rows, _ = block_refs[0].shape
    tiles = sems.shape[1]
    tile = held.shape[1] // tiles
    copies = []
    for v in range(size):
        for k, block in enumerate(block_refs):
            rhs[v, k * rows : (k + 1) * rows, :] = block[v]
        for t in range(tiles):
            part = pl.ds(t * tile, tile)
            total = near_ref[first + v, part, :] + jnp.dot(
                lhs_ref[part, :], rhs[v], preferred_element_type=jnp.float32
            )
            held[v, part, :] = total.astype(held.dtype)
            copy = pltpu.make_async_copy(
                held.at[v, part, :], out_ref.at[first + v, part, :], sems.at[v, t]
            )
            copy.start()
            copies.append(copy)
    for copy in copies:
        copy.wait()


def far_sum(lhs, near, blocks, rotated, first):
    size, _, columns = blocks[0].shape
    occupied, depth = lhs.shape
    tiles = 4
    given = [] if rotated is None else [rotated]
    whole, left = pl.BlockSpec(memory_space=pltpu.VMEM), pl.BlockSpec(memory_space=pl.ANY)
    return pl.pallas_call(
        functools.partial(far_kernel, first, len(blocks)),
        out_shape=jax.ShapeDtypeStruct(near.shape, jnp.bfloat16),
        in_specs=[whole] * (2 + len(blocks)) + [left] * len(given),
        out_specs=left,
        scratch_shapes=[
            pltpu.VMEM((size, depth, columns), jnp.bfloat16),
            pltpu.VMEM((size, occupied, columns), jnp.bfloat16),
            pltpu.SemaphoreType.DMA((size, tiles)),
        ],
        input_output_aliases={2 + len(blocks): 0} if given else {},
        compiler_params=params(20),
        cost_estimate=cost(2 * size * occupied * depth * columns, 4 * size * occupied * columns),
        name="far",
    )(lhs, near, *blocks, *given)


def local(owners, chol, orbitals, greens, shift):
    walkers = greens.shape[2] // chol.shape[2]
    count = chol.shape[0] // owners
    rows, columns = chol.shape[1:]
    me, mine = lax.axis_index("orb"), lax.axis_index("walk")
    first, second, far_offsets = offsets(owners)

    def swap(value, axis, k, size):
        return lax.ppermute(value, axis, [(i, i ^ k) for i in range(size)])

    def part(source, k, start=0, stop=count):
        return lax.dynamic_slice_in_dim(source, (me ^ k) * count + start, stop - start, 0)

    source, near = chol, {k: [] for k in first}
    for start, stop in ((0, 1), (1, count)):
        pieces = [part(source, k, start, stop) for k in first]
        source, orbitals, greens = tied((source, orbitals, greens), *pieces)
        for k, piece in zip(first, pieces):
            near[k].append(swap(piece, "orb", k, owners))

    orbital_rows = lax.dynamic_slice_in_dim(orbitals, me * rows, rows, 0)
    products = jnp.dot(orbital_rows, greens[0], preferred_element_type=jnp.float32)
    products = products.astype(jnp.bfloat16)
    pieces = [
        lax.dynamic_slice_in_dim(products, (mine ^ k) * columns, columns, 1) for k in range(walkers)
    ]
    source = tied(source, *pieces)
    arrived = pieces[:1] + [swap(pieces[k], "walk", k, walkers) for k in range(1, walkers)]

    pieces = {k: part(source, k) for k in [0] + second}
    source = tied(source, *pieces.values())
    near[0] = [pieces[0]]
    for k in second:
        near[k] = [swap(pieces[k], "orb", k, owners)]

    cuts = [0, max(count - 2, 0), count - 1, count]
    cuts = [(a, b) for a, b in zip(cuts, cuts[1:]) if a < b]
    pieces = [part(source, k, *cuts[0]) for k in far_offsets]
    far = [[swap(piece, "orb", k, owners) for k, piece in zip(far_offsets, pieces)]]

    order = [0] + first + second
    lhs_near = turned(orbitals, jnp.array(order, jnp.int32) ^ me, rows)
    lhs_far = turned(orbitals, jnp.array(far_offsets, jnp.int32) ^ me, rows)

    terms = force_terms(chol, arrived, jnp.stack([me, mine]).astype(jnp.int32), count)
    terms = terms.sum(axis=(2, 3))
    total = terms[0] + sum(swap(terms[k], "walk", k, walkers) for k in range(1, walkers))
    total = total.reshape(owners, count)
    even = total[0::2] + swap(total[1::2], "orb", 1, owners)
    sums = [swap(even[k : k + 1], "orb", 2 * k, owners) for k in range(1, owners // 2)]

    source = tied(source, even)
    for cut in cuts[1:]:
        far.append([swap(part(source, k, *cut), "orb", k, owners) for k in far_offsets])

    partial = near_sum(lhs_near, [near[k] for k in order])
    sums = tied(sums, partial)
    force_bias = even[:1] + sum(sums) - shift[None, :]
    rotated = None
    for (start, _), blocks in zip(cuts, far):
        rotated = far_sum(lhs_far, partial, blocks, rotated, start)
    return force_bias, rotated


def solution(mesh):
    in_specs = (P(None, "orb", "walk"), P(), P("walk", None, None), P("orb"))
    out_specs = (P("walk", "orb"), P("orb", None, "walk"))
    owners = mesh.shape["orb"]

    def body(*args):
        return local(owners, *args)

    return jax.shard_map(body, mesh=mesh, in_specs=in_specs, out_specs=out_specs, check_vma=False)
```

```python
import functools

import jax
import jax.numpy as jnp
from jax import lax
from jax.experimental import pallas as pl
from jax.experimental.pallas import tpu as pltpu
from jax.sharding import PartitionSpec as P


MIB = 2**20


def tied(value, *after):
    return lax.optimization_barrier((value, *after))[0]


def in_hbm(value):
    return pltpu.with_memory_space_constraint(value, pltpu.HBM)


def params(mib):
    return pltpu.CompilerParams(vmem_limit_bytes=mib * MIB)


def offsets(owners):
    chips = lambda k: (k >> 1).bit_count()
    first = [k for k in range(owners - 2, 0, -2) if chips(k) == 1]
    second = [k + 1 for k in first] + [1]
    return first, second, [k for k in range(1, owners) if chips(k) > 1]


def last_parts(columns):
    return 2 if columns % 256 == 0 else 1


def cost(flops, moved):
    return pl.CostEstimate(flops=flops, bytes_accessed=moved, transcendentals=0)


def first_kernel(offsets, count, chol_ref, *refs):
    out_refs, sems = refs[:-1], refs[-1]
    me = lax.axis_index("orb")
    copies = []
    for n, (k, out_ref) in enumerate(zip(offsets, out_refs)):
        piece = chol_ref.at[pl.ds((me ^ k) * count, out_ref.shape[0])]
        copies.append(pltpu.make_async_copy(piece, out_ref, sems.at[n]))
        copies[-1].start()
    for copy in copies:
        copy.wait()


def first_pieces(chol, offsets, count, size):
    shape = jax.ShapeDtypeStruct((size,) + chol.shape[1:], chol.dtype)
    return pl.pallas_call(
        functools.partial(first_kernel, offsets, count),
        out_shape=[shape] * len(offsets),
        in_specs=[pl.BlockSpec(memory_space=pl.ANY)],
        out_specs=[pl.BlockSpec(memory_space=pltpu.VMEM)] * len(offsets),
        scratch_shapes=[pltpu.SemaphoreType.DMA((len(offsets),))],
        compiler_params=params(8),
        cost_estimate=cost(2**20, 4 * len(offsets) * size * chol[0].size),
        name="first",
    )(in_hbm(chol))


def terms_kernel(place, chol_ref, *refs):
    product_refs, out_ref = refs[:-1], refs[-1]
    for v in range(chol_ref.shape[0]):
        block = chol_ref[v].astype(jnp.float32)
        for w, product in enumerate(product_refs):
            terms = jnp.sum(product[...].astype(jnp.float32) * block, axis=0, keepdims=True)
            out_ref[w, v] = terms


def force_terms(chol, products, me, count):
    vectors, rows, columns = chol.shape
    walkers = len(products)
    whole = pl.BlockSpec((rows, columns), lambda v, place: (0, 0))
    return pl.pallas_call(
        terms_kernel,
        out_shape=jax.ShapeDtypeStruct((walkers, vectors, 1, columns), jnp.float32),
        grid_spec=pltpu.PrefetchScalarGridSpec(
            num_scalar_prefetch=1,
            grid=(vectors // count,),
            in_specs=[pl.BlockSpec((count, rows, columns), lambda v, place: (place[0] ^ v, 0, 0))]
            + [whole] * walkers,
            out_specs=pl.BlockSpec((walkers, count, 1, columns), lambda v, place: (0, v, 0, 0)),
        ),
        compiler_params=params(12),
        cost_estimate=cost(2 * walkers * chol.size, 2 * chol.size),
        name="terms",
    )(me, in_hbm(chol), *products)


def turn_kernel(place, source_ref, out_ref):
    out_ref[...] = source_ref[...].T


def turned(orbitals, owners, rows):
    occupied = orbitals.shape[1]
    blocks = owners.shape[0]
    return pl.pallas_call(
        turn_kernel,
        out_shape=jax.ShapeDtypeStruct((occupied, blocks * rows), orbitals.dtype),
        grid_spec=pltpu.PrefetchScalarGridSpec(
            num_scalar_prefetch=1,
            grid=(blocks,),
            in_specs=[pl.BlockSpec((rows, occupied), lambda k, place: (place[k], 0))],
            out_specs=pl.BlockSpec((occupied, rows), lambda k, place: (0, k)),
        ),
        compiler_params=params(8),
        cost_estimate=cost(blocks * rows * occupied * 300, 4 * blocks * rows * occupied),
        name="turn",
    )(owners, orbitals)


def near_kernel(counts, lhs_ref, *refs):
    piece_refs, out_ref, rhs = refs[:-2], refs[-2], refs[-1]
    rows = piece_refs[0].shape[1]
    vector = pl.program_id(0)
    piece_refs = iter(piece_refs)
    for k, pieces in enumerate(counts):
        at, start = pl.ds(k * rows, rows), 0
        for size in pieces:
            piece = next(piece_refs)

            @pl.when((vector >= start) & (vector < start + size))
            def _():
                rhs[at, :] = piece[0]

            start += size
    out_ref[0] = jnp.dot(lhs_ref[...], rhs[...], preferred_element_type=jnp.float32)


def near_sum(lhs, blocks):
    counts = [[piece.shape[0] for piece in pieces] for pieces in blocks]
    count, (_, rows, columns) = sum(counts[0]), blocks[0][0].shape
    occupied, depth = lhs.shape
    specs = [pl.BlockSpec((occupied, depth), lambda g: (0, 0))]
    for pieces in counts:
        start = 0
        for size in pieces:
            at = functools.partial(lambda start, size, g: (jnp.clip(g - start, 0, size - 1), 0, 0), start, size)
            specs.append(pl.BlockSpec((1, rows, columns), at))
            start += size
    return pl.pallas_call(
        functools.partial(near_kernel, counts),
        out_shape=jax.ShapeDtypeStruct((count, occupied, columns), jnp.float32),
        grid=(count,),
        in_specs=specs,
        out_specs=pl.BlockSpec((1, occupied, columns), lambda g: (g, 0, 0)),
        scratch_shapes=[pltpu.VMEM((depth, columns), jnp.bfloat16)],
        compiler_params=params(24),
        cost_estimate=cost(2 * count * occupied * depth * columns, 4 * count * occupied * columns),
        name="near",
    )(in_hbm(lhs), *(in_hbm(piece) for pieces in blocks for piece in pieces))


def far_kernel(first, blocks, lhs_ref, near_ref, *refs):
    block_refs, (out_ref, rhs, held, sems) = refs[:blocks], refs[-4:]
    size, rows, _ = block_refs[0].shape
    tiles = sems.shape[1]
    tile = held.shape[1] // tiles
    copies = []
    for v in range(size):
        for k, block in enumerate(block_refs):
            rhs[v, k * rows : (k + 1) * rows, :] = block[v]
        for t in range(tiles):
            part = pl.ds(t * tile, tile)
            total = near_ref[first + v, part, :] + jnp.dot(
                lhs_ref[part, :], rhs[v], preferred_element_type=jnp.float32
            )
            held[v, part, :] = total.astype(held.dtype)
            copy = pltpu.make_async_copy(
                held.at[v, part, :], out_ref.at[first + v, part, :], sems.at[v, t]
            )
            copy.start()
            copies.append(copy)
    for copy in copies:
        copy.wait()


def far_sum(lhs, near, blocks, rotated, first):
    size, _, columns = blocks[0].shape
    occupied, depth = lhs.shape
    tiles = 4
    given = [] if rotated is None else [rotated]
    whole, left = pl.BlockSpec(memory_space=pltpu.VMEM), pl.BlockSpec(memory_space=pl.ANY)
    return pl.pallas_call(
        functools.partial(far_kernel, first, len(blocks)),
        out_shape=jax.ShapeDtypeStruct(near.shape, jnp.bfloat16),
        in_specs=[whole] * (2 + len(blocks)) + [left] * len(given),
        out_specs=left,
        scratch_shapes=[
            pltpu.VMEM((size, depth, columns), jnp.bfloat16),
            pltpu.VMEM((size, occupied, columns), jnp.bfloat16),
            pltpu.SemaphoreType.DMA((size, tiles)),
        ],
        input_output_aliases={2 + len(blocks): 0} if given else {},
        compiler_params=params(20),
        cost_estimate=cost(2 * size * occupied * depth * columns, 4 * size * occupied * columns),
        name="far",
    )(lhs, near, *blocks, *given)


def middle_kernel(vector, lhs_ref, near_ref, *refs):
    block_refs, out_ref = refs[:-1], refs[-1]
    rows = block_refs[0].shape[1]
    tile = out_ref.shape[0] // 4
    for t in range(4):
        at = pl.ds(t * tile, tile)
        total = near_ref[vector, at, :]
        for k, block in enumerate(block_refs):
            total += jnp.dot(
                lhs_ref[at, k * rows : (k + 1) * rows], block[0], preferred_element_type=jnp.float32
            )
        out_ref[at, :] = total


def middle_sum(lhs, near, blocks, vector):
    _, rows, columns = blocks[0].shape
    occupied = lhs.shape[0]
    return pl.pallas_call(
        functools.partial(middle_kernel, vector),
        out_shape=jax.ShapeDtypeStruct((occupied, columns), jnp.float32),
        in_specs=[pl.BlockSpec(memory_space=pltpu.VMEM)] * (2 + len(blocks)),
        out_specs=pl.BlockSpec(memory_space=pltpu.VMEM),
        compiler_params=params(16),
        cost_estimate=cost(2 * occupied * rows * columns * len(blocks), 8 * occupied * columns),
        name="middle",
    )(lhs, near, *blocks)


def last_kernel(vector, start, lhs_ref, near_ref, block_ref, _, out_ref, held, sems):
    _, rows, columns = block_ref.shape
    at_columns, weights = pl.ds(start, columns), pl.ds(lhs_ref.shape[1] - rows, rows)
    tiles = sems.shape[0]
    tile = held.shape[0] // tiles
    copies = []
    for t in range(tiles):
        at = pl.ds(t * tile, tile)
        total = near_ref[at, at_columns] + jnp.dot(
            lhs_ref[at, weights], block_ref[0], preferred_element_type=jnp.float32
        )
        held[at, :] = total.astype(held.dtype)
        copies.append(
            pltpu.make_async_copy(held.at[at, :], out_ref.at[vector, at, at_columns], sems.at[t])
        )
        copies[-1].start()
    for copy in copies:
        copy.wait()


def last_sum(lhs, near, block, rotated, vector, start):
    _, rows, columns = block.shape
    occupied, tiles = lhs.shape[0], 8
    whole, left = pl.BlockSpec(memory_space=pltpu.VMEM), pl.BlockSpec(memory_space=pl.ANY)
    return pl.pallas_call(
        functools.partial(last_kernel, vector, start),
        out_shape=jax.ShapeDtypeStruct(rotated.shape, rotated.dtype),
        in_specs=[whole, whole, whole, left],
        out_specs=left,
        scratch_shapes=[
            pltpu.VMEM((occupied, columns), rotated.dtype),
            pltpu.SemaphoreType.DMA((tiles,)),
        ],
        input_output_aliases={3: 0},
        compiler_params=params(16),
        cost_estimate=cost(2 * occupied * rows * columns, 4 * occupied * columns),
        name="last",
    )(lhs, near, block, rotated)


def local(owners, chol, orbitals, greens, shift):
    walkers = greens.shape[2] // chol.shape[2]
    count = chol.shape[0] // owners
    rows, columns = chol.shape[1:]
    me, mine = lax.axis_index("orb"), lax.axis_index("walk")
    first, second, far_offsets = offsets(owners)

    def swap(value, axis, k, size):
        return lax.ppermute(value, axis, [(i, i ^ k) for i in range(size)])

    def part(source, k, start=0, stop=count):
        return lax.dynamic_slice_in_dim(source, (me ^ k) * count + start, stop - start, 0)

    source, near = chol, {k: [] for k in first}
    for start, stop in ((0, 1), (1, count)):
        if start == 0:
            pieces = first_pieces(chol, first, count, stop)
        else:
            pieces = [part(source, k, start, stop) for k in first]
        source, orbitals, greens = tied((source, orbitals, greens), *pieces)
        for k, piece in zip(first, pieces):
            near[k].append(swap(piece, "orb", k, owners))

    pieces = {k: part(source, k) for k in [0] + second}
    source = tied(source, *pieces.values())
    near[0] = [pieces[0]]
    for k in second:
        near[k] = [swap(pieces[k], "orb", k, owners)]

    arrived = [near[k][0] for k in first]
    orbitals, greens = tied((orbitals, greens), *pieces.values(), *arrived)
    orbital_rows = lax.dynamic_slice_in_dim(orbitals, me * rows, rows, 0)
    products = jnp.dot(orbital_rows, greens[0], preferred_element_type=jnp.float32)
    products = products.astype(jnp.bfloat16)
    pieces = [
        lax.dynamic_slice_in_dim(products, (mine ^ k) * columns, columns, 1) for k in range(walkers)
    ]
    source = tied(source, *pieces)
    arrived = pieces[:1] + [swap(pieces[k], "walk", k, walkers) for k in range(1, walkers)]

    cuts = [(a, b) for a, b in ((0, count - 2), (count - 2, count - 1)) if a < b]
    far = []
    for span in cuts:
        pieces = [part(source, k, *span) for k in far_offsets]
        source = tied(source, *pieces)
        far.append([swap(piece, "orb", k, owners) for k, piece in zip(far_offsets, pieces)])

    order = [0] + first + second
    lhs_near = turned(orbitals, jnp.array(order, jnp.int32) ^ me, rows)
    lhs_far = turned(orbitals, jnp.array(far_offsets, jnp.int32) ^ me, rows)

    terms = force_terms(chol, arrived, jnp.stack([me, mine]).astype(jnp.int32), count)
    terms = terms.sum(axis=(2, 3))
    total = terms[0] + sum(swap(terms[k], "walk", k, walkers) for k in range(1, walkers))
    total = total.reshape(owners, count)
    even = total[0::2] + swap(total[1::2], "orb", 1, owners)
    sums = [swap(even[k : k + 1], "orb", 2 * k, owners) for k in range(1, owners // 2)]

    source = tied(source, even)
    pieces = [part(source, k, count - 1) for k in far_offsets]
    middle = [swap(piece, "orb", k, owners) for k, piece in zip(far_offsets[:-1], pieces)]
    half = columns // last_parts(columns)
    last = [
        swap(pieces[-1][..., at : at + half], "orb", far_offsets[-1], owners)
        for at in range(0, columns, half)
    ]

    partial = near_sum(lhs_near, [near[k] for k in order])
    sums = tied(sums, partial)
    force_bias = even[:1] + sum(sums) - shift[None, :]
    rotated = None
    for (start, _), blocks in zip(cuts, far):
        rotated = far_sum(lhs_far, partial, blocks, rotated, start)
    partial = middle_sum(lhs_far, partial, middle, count - 1)
    for n, block in enumerate(last):
        rotated = last_sum(lhs_far, partial, block, rotated, count - 1, n * half)
    return force_bias, rotated


def solution(mesh):
    in_specs = (P(None, "orb", "walk"), P(), P("walk", None, None), P("orb"))
    out_specs = (P("walk", "orb"), P("orb", None, "walk"))
    owners = mesh.shape["orb"]

    def step(chol, *args):
        def body(*args):
            return local(owners, *args)

        run = jax.shard_map(
            body, mesh=mesh, in_specs=in_specs, out_specs=out_specs, check_vma=False
        )
        return run(chol, *args)

    return step
```

```python
import functools

import jax
import jax.numpy as jnp
from jax import lax
from jax.experimental import pallas as pl
from jax.experimental.pallas import tpu as pltpu
from jax.sharding import PartitionSpec as P


MIB = 2**20


def tied(value, *after):
    return lax.optimization_barrier((value, *after))[0]


def in_hbm(value):
    return pltpu.with_memory_space_constraint(value, pltpu.HBM)


def params(mib):
    return pltpu.CompilerParams(vmem_limit_bytes=mib * MIB)


def offsets(owners):
    chips = lambda k: (k >> 1).bit_count()
    first = [k for k in range(owners - 2, 0, -2) if chips(k) == 1]
    second = [k + 1 for k in first] + [1]
    return first, second, [k for k in range(1, owners) if chips(k) > 1]


def last_parts(columns):
    return 2 if columns % 256 == 0 else 1


def cost(flops, moved):
    return pl.CostEstimate(flops=flops, bytes_accessed=moved, transcendentals=0)


def first_kernel(offsets, count, chol_ref, *refs):
    out_refs, sems = refs[:-1], refs[-1]
    me = lax.axis_index("orb")
    copies = []
    for n, (k, out_ref) in enumerate(zip(offsets, out_refs)):
        piece = chol_ref.at[pl.ds((me ^ k) * count, out_ref.shape[0])]
        copies.append(pltpu.make_async_copy(piece, out_ref, sems.at[n]))
        copies[-1].start()
    for copy in copies:
        copy.wait()


def first_pieces(chol, offsets, count, size):
    shape = jax.ShapeDtypeStruct((size,) + chol.shape[1:], chol.dtype)
    return pl.pallas_call(
        functools.partial(first_kernel, offsets, count),
        out_shape=[shape] * len(offsets),
        in_specs=[pl.BlockSpec(memory_space=pl.ANY)],
        out_specs=[pl.BlockSpec(memory_space=pltpu.VMEM)] * len(offsets),
        scratch_shapes=[pltpu.SemaphoreType.DMA((len(offsets),))],
        compiler_params=params(8),
        cost_estimate=cost(2**20, 4 * len(offsets) * size * chol[0].size),
        name="first",
    )(in_hbm(chol))


def terms_kernel(place, chol_ref, *refs):
    product_refs, out_ref = refs[:-1], refs[-1]
    for v in range(chol_ref.shape[0]):
        block = chol_ref[v].astype(jnp.float32)
        for w, product in enumerate(product_refs):
            terms = jnp.sum(product[...].astype(jnp.float32) * block, axis=0, keepdims=True)
            out_ref[w, v] = terms


def force_terms(chol, products, me, count):
    vectors, rows, columns = chol.shape
    walkers = len(products)
    whole = pl.BlockSpec((rows, columns), lambda v, place: (0, 0))
    return pl.pallas_call(
        terms_kernel,
        out_shape=jax.ShapeDtypeStruct((walkers, vectors, 1, columns), jnp.float32),
        grid_spec=pltpu.PrefetchScalarGridSpec(
            num_scalar_prefetch=1,
            grid=(vectors // count,),
            in_specs=[pl.BlockSpec((count, rows, columns), lambda v, place: (place[0] ^ v, 0, 0))]
            + [whole] * walkers,
            out_specs=pl.BlockSpec((walkers, count, 1, columns), lambda v, place: (0, v, 0, 0)),
        ),
        compiler_params=params(12),
        cost_estimate=cost(2 * walkers * chol.size, 2 * chol.size),
        name="terms",
    )(me, in_hbm(chol), *products)


def turn_kernel(place, source_ref, out_ref):
    out_ref[...] = source_ref[...].T


def turned(orbitals, owners, rows):
    occupied = orbitals.shape[1]
    blocks = owners.shape[0]
    return pl.pallas_call(
        turn_kernel,
        out_shape=jax.ShapeDtypeStruct((occupied, blocks * rows), orbitals.dtype),
        grid_spec=pltpu.PrefetchScalarGridSpec(
            num_scalar_prefetch=1,
            grid=(blocks,),
            in_specs=[pl.BlockSpec((rows, occupied), lambda k, place: (place[k], 0))],
            out_specs=pl.BlockSpec((occupied, rows), lambda k, place: (0, k)),
        ),
        compiler_params=params(8),
        cost_estimate=cost(blocks * rows * occupied * 300, 4 * blocks * rows * occupied),
        name="turn",
    )(owners, orbitals)


def near_kernel(counts, lhs_ref, *refs):
    piece_refs, out_ref, rhs = refs[:-2], refs[-2], refs[-1]
    rows = piece_refs[0].shape[1]
    vector = pl.program_id(0)
    piece_refs = iter(piece_refs)
    for k, pieces in enumerate(counts):
        at, start = pl.ds(k * rows, rows), 0
        for size in pieces:
            piece = next(piece_refs)

            @pl.when((vector >= start) & (vector < start + size))
            def _():
                rhs[at, :] = piece[0]

            start += size
    out_ref[0] = jnp.dot(lhs_ref[...], rhs[...], preferred_element_type=jnp.float32)


def near_sum(lhs, blocks):
    counts = [[piece.shape[0] for piece in pieces] for pieces in blocks]
    count, (_, rows, columns) = sum(counts[0]), blocks[0][0].shape
    occupied, depth = lhs.shape
    specs = [pl.BlockSpec((occupied, depth), lambda g: (0, 0))]
    for pieces in counts:
        start = 0
        for size in pieces:
            at = functools.partial(lambda start, size, g: (jnp.clip(g - start, 0, size - 1), 0, 0), start, size)
            specs.append(pl.BlockSpec((1, rows, columns), at))
            start += size
    return pl.pallas_call(
        functools.partial(near_kernel, counts),
        out_shape=jax.ShapeDtypeStruct((count, occupied, columns), jnp.float32),
        grid=(count,),
        in_specs=specs,
        out_specs=pl.BlockSpec((1, occupied, columns), lambda g: (g, 0, 0)),
        scratch_shapes=[pltpu.VMEM((depth, columns), jnp.bfloat16)],
        compiler_params=params(24),
        cost_estimate=cost(2 * count * occupied * depth * columns, 4 * count * occupied * columns),
        name="near",
    )(in_hbm(lhs), *(in_hbm(piece) for pieces in blocks for piece in pieces))


def far_kernel(lhs_ref, near_ref, *refs):
    block_refs, (out_ref, rhs, held, sems) = refs[:-4], refs[-4:]
    size, rows, _ = block_refs[0].shape
    tiles = sems.shape[1]
    tile = held.shape[1] // tiles
    copies = []
    for v in range(size):
        for k, block in enumerate(block_refs):
            rhs[v, k * rows : (k + 1) * rows, :] = block[v]
        for t in range(tiles):
            at = pl.ds(t * tile, tile)
            total = near_ref[v, at, :] + jnp.dot(
                lhs_ref[at, :], rhs[v], preferred_element_type=jnp.float32
            )
            held[v, at, :] = total.astype(held.dtype)
            copies.append(pltpu.make_async_copy(held.at[v, at, :], out_ref.at[v, at, :], sems.at[v, t]))
            copies[-1].start()
    for copy in copies:
        copy.wait()


def far_sum(lhs, near, blocks):
    size, _, columns = blocks[0].shape
    occupied, depth = lhs.shape
    tiles = 4
    return pl.pallas_call(
        far_kernel,
        out_shape=jax.ShapeDtypeStruct(near.shape, jnp.bfloat16),
        in_specs=[pl.BlockSpec(memory_space=pltpu.VMEM)] * (2 + len(blocks)),
        out_specs=pl.BlockSpec(memory_space=pl.ANY),
        scratch_shapes=[
            pltpu.VMEM((size, depth, columns), jnp.bfloat16),
            pltpu.VMEM((size, occupied, columns), jnp.bfloat16),
            pltpu.SemaphoreType.DMA((size, tiles)),
        ],
        compiler_params=params(20),
        cost_estimate=cost(2 * size * occupied * depth * columns, 4 * size * occupied * columns),
        name="far",
    )(lhs, near, *blocks)


def middle_kernel(vector, lhs_ref, near_ref, *refs):
    block_refs, out_ref = refs[:-1], refs[-1]
    rows = block_refs[0].shape[1]
    tile = out_ref.shape[0] // 4
    for t in range(4):
        at = pl.ds(t * tile, tile)
        total = near_ref[vector, at, :]
        for k, block in enumerate(block_refs):
            total += jnp.dot(
                lhs_ref[at, k * rows : (k + 1) * rows], block[0], preferred_element_type=jnp.float32
            )
        out_ref[at, :] = total


def middle_sum(lhs, near, blocks, vector):
    _, rows, columns = blocks[0].shape
    occupied = lhs.shape[0]
    return pl.pallas_call(
        functools.partial(middle_kernel, vector),
        out_shape=jax.ShapeDtypeStruct((occupied, columns), jnp.float32),
        in_specs=[pl.BlockSpec(memory_space=pltpu.VMEM)] * (2 + len(blocks)),
        out_specs=pl.BlockSpec(memory_space=pltpu.VMEM),
        compiler_params=params(16),
        cost_estimate=cost(2 * occupied * rows * columns * len(blocks), 8 * occupied * columns),
        name="middle",
    )(lhs, near, *blocks)


def last_kernel(vector, start, lhs_ref, near_ref, block_ref, _, out_ref, held, sems):
    _, rows, columns = block_ref.shape
    at_columns, weights = pl.ds(start, columns), pl.ds(lhs_ref.shape[1] - rows, rows)
    tiles = sems.shape[0]
    tile = held.shape[0] // tiles
    copies = []
    for t in range(tiles):
        at = pl.ds(t * tile, tile)
        total = near_ref[at, at_columns] + jnp.dot(
            lhs_ref[at, weights], block_ref[0], preferred_element_type=jnp.float32
        )
        held[at, :] = total.astype(held.dtype)
        copies.append(
            pltpu.make_async_copy(held.at[at, :], out_ref.at[vector, at, at_columns], sems.at[t])
        )
        copies[-1].start()
    for copy in copies:
        copy.wait()


def last_sum(lhs, near, block, rotated, vector, start):
    _, rows, columns = block.shape
    occupied, tiles = lhs.shape[0], 8
    whole, left = pl.BlockSpec(memory_space=pltpu.VMEM), pl.BlockSpec(memory_space=pl.ANY)
    return pl.pallas_call(
        functools.partial(last_kernel, vector, start),
        out_shape=jax.ShapeDtypeStruct(rotated.shape, rotated.dtype),
        in_specs=[whole, whole, whole, left],
        out_specs=left,
        scratch_shapes=[
            pltpu.VMEM((occupied, columns), rotated.dtype),
            pltpu.SemaphoreType.DMA((tiles,)),
        ],
        input_output_aliases={3: 0},
        compiler_params=params(16),
        cost_estimate=cost(2 * occupied * rows * columns, 4 * occupied * columns),
        name="last",
    )(lhs, near, block, rotated)


def local(owners, chol, orbitals, greens, shift):
    walkers = greens.shape[2] // chol.shape[2]
    count = chol.shape[0] // owners
    rows, columns = chol.shape[1:]
    me, mine = lax.axis_index("orb"), lax.axis_index("walk")
    first, second, far_offsets = offsets(owners)

    def swap(value, axis, k, size):
        return lax.ppermute(value, axis, [(i, i ^ k) for i in range(size)])

    def part(source, k, start=0, stop=count):
        return lax.dynamic_slice_in_dim(source, (me ^ k) * count + start, stop - start, 0)

    source, near = chol, {k: [] for k in first}
    for start, stop in ((0, 1), (1, count)):
        if start == 0:
            pieces = first_pieces(chol, first, count, stop)
        else:
            pieces = [part(source, k, start, stop) for k in first]
        source, orbitals, greens = tied((source, orbitals, greens), *pieces)
        for k, piece in zip(first, pieces):
            near[k].append(swap(piece, "orb", k, owners))

    pieces = {k: part(source, k) for k in [0] + second}
    source = tied(source, *pieces.values())
    near[0] = [pieces[0]]
    for k in second:
        near[k] = [swap(pieces[k], "orb", k, owners)]

    arrived = [near[k][0] for k in first]
    orbitals, greens = tied((orbitals, greens), *pieces.values(), *arrived)
    orbital_rows = lax.dynamic_slice_in_dim(orbitals, me * rows, rows, 0)
    products = jnp.dot(orbital_rows, greens[0], preferred_element_type=jnp.float32)
    products = products.astype(jnp.bfloat16)
    pieces = [
        lax.dynamic_slice_in_dim(products, (mine ^ k) * columns, columns, 1) for k in range(walkers)
    ]
    source = tied(source, *pieces)
    arrived = pieces[:1] + [swap(pieces[k], "walk", k, walkers) for k in range(1, walkers)]

    pieces = [part(source, k, 0, count - 1) for k in far_offsets]
    source = tied(source, *pieces)
    far = [swap(piece, "orb", k, owners) for k, piece in zip(far_offsets, pieces)]

    order = [0] + first + second
    lhs_near = turned(orbitals, jnp.array(order, jnp.int32) ^ me, rows)
    lhs_far = turned(orbitals, jnp.array(far_offsets, jnp.int32) ^ me, rows)

    terms = force_terms(chol, arrived, jnp.stack([me, mine]).astype(jnp.int32), count)
    terms = terms.sum(axis=(2, 3))
    total = terms[0] + sum(swap(terms[k], "walk", k, walkers) for k in range(1, walkers))
    total = total.reshape(owners, count)
    even = total[0::2] + swap(total[1::2], "orb", 1, owners)
    sums = [swap(even[k : k + 1], "orb", 2 * k, owners) for k in range(1, owners // 2)]

    source = tied(source, even)
    pieces = [part(source, k, count - 1) for k in far_offsets]
    middle = [swap(piece, "orb", k, owners) for k, piece in zip(far_offsets[:-1], pieces)]
    half = columns // last_parts(columns)
    last = [
        swap(pieces[-1][..., at : at + half], "orb", far_offsets[-1], owners)
        for at in range(0, columns, half)
    ]

    partial = near_sum(lhs_near, [near[k] for k in order])
    sums = tied(sums, partial)
    force_bias = even[:1] + sum(sums) - shift[None, :]
    rotated = far_sum(lhs_far, partial, far)
    partial = middle_sum(lhs_far, partial, middle, count - 1)
    for n, block in enumerate(last):
        rotated = last_sum(lhs_far, partial, block, rotated, count - 1, n * half)
    return force_bias, rotated


def solution(mesh):
    in_specs = (P(None, "orb", "walk"), P(), P("walk", None, None), P("orb"))
    out_specs = (P("walk", "orb"), P("orb", None, "walk"))
    owners = mesh.shape["orb"]

    def step(chol, *args):
        def body(*args):
            return local(owners, *args)

        run = jax.shard_map(
            body, mesh=mesh, in_specs=in_specs, out_specs=out_specs, check_vma=False
        )
        return run(chol, *args)

    return step
```

```python
import functools

import jax
import jax.numpy as jnp
from jax import lax
from jax.experimental import pallas as pl
from jax.experimental.pallas import tpu as pltpu
from jax.sharding import PartitionSpec as P


MIB = 2**20


def tied(value, *after):
    return lax.optimization_barrier((value, *after))[0]


def params(mib):
    return pltpu.CompilerParams(vmem_limit_bytes=mib * MIB)


def offsets(owners):
    chips = lambda k: (k >> 1).bit_count()
    first = [k for k in range(owners - 2, 0, -2) if chips(k) == 1]
    second = [k + 1 for k in first] + [1]
    return first, second, [k for k in range(1, owners) if chips(k) > 1]


def last_parts(columns):
    return 2 if columns % 256 == 0 else 1


def cost(flops, moved):
    return pl.CostEstimate(flops=flops, bytes_accessed=moved, transcendentals=0)


def first_kernel(offsets, count, chol_ref, *refs):
    out_refs, sems = refs[:-1], refs[-1]
    me = lax.axis_index("orb")
    copies = []
    for n, (k, out_ref) in enumerate(zip(offsets, out_refs)):
        piece = chol_ref.at[pl.ds((me ^ k) * count, out_ref.shape[0])]
        copies.append(pltpu.make_async_copy(piece, out_ref, sems.at[n]))
        copies[-1].start()
    for copy in copies:
        copy.wait()


def first_pieces(chol, offsets, count, size):
    shape = jax.ShapeDtypeStruct((size,) + chol.shape[1:], chol.dtype)
    return pl.pallas_call(
        functools.partial(first_kernel, offsets, count),
        out_shape=[shape] * len(offsets),
        in_specs=[pl.BlockSpec(memory_space=pl.ANY)],
        out_specs=[pl.BlockSpec(memory_space=pltpu.VMEM)] * len(offsets),
        scratch_shapes=[pltpu.SemaphoreType.DMA((len(offsets),))],
        compiler_params=params(8),
        cost_estimate=cost(2**20, 4 * len(offsets) * size * chol[0].size),
        name="first",
    )(pltpu.with_memory_space_constraint(chol, pltpu.HBM))


def terms_kernel(place, chol_ref, *refs):
    product_refs, out_ref = refs[:-1], refs[-1]
    for v in range(chol_ref.shape[0]):
        block = chol_ref[v].astype(jnp.float32)
        for w, product in enumerate(product_refs):
            terms = jnp.sum(product[...].astype(jnp.float32) * block, axis=0, keepdims=True)
            out_ref[w, v] = terms


def force_terms(chol, products, me, count):
    vectors, rows, columns = chol.shape
    walkers = len(products)
    whole = pl.BlockSpec((rows, columns), lambda v, place: (0, 0))
    return pl.pallas_call(
        terms_kernel,
        out_shape=jax.ShapeDtypeStruct((walkers, vectors, 1, columns), jnp.float32),
        grid_spec=pltpu.PrefetchScalarGridSpec(
            num_scalar_prefetch=1,
            grid=(vectors // count,),
            in_specs=[pl.BlockSpec((count, rows, columns), lambda v, place: (place[0] ^ v, 0, 0))]
            + [whole] * walkers,
            out_specs=pl.BlockSpec((walkers, count, 1, columns), lambda v, place: (0, v, 0, 0)),
        ),
        compiler_params=params(12),
        cost_estimate=cost(2 * walkers * chol.size, 2 * chol.size),
        name="terms",
    )(me, pltpu.with_memory_space_constraint(chol, pltpu.HBM), *products)


def turn_kernel(place, source_ref, out_ref):
    out_ref[...] = source_ref[...].T


def turned(orbitals, owners, rows):
    occupied = orbitals.shape[1]
    blocks = owners.shape[0]
    return pl.pallas_call(
        turn_kernel,
        out_shape=jax.ShapeDtypeStruct((occupied, blocks * rows), orbitals.dtype),
        grid_spec=pltpu.PrefetchScalarGridSpec(
            num_scalar_prefetch=1,
            grid=(blocks,),
            in_specs=[pl.BlockSpec((rows, occupied), lambda k, place: (place[k], 0))],
            out_specs=pl.BlockSpec((occupied, rows), lambda k, place: (0, k)),
        ),
        compiler_params=params(8),
        cost_estimate=cost(blocks * rows * occupied * 300, 4 * blocks * rows * occupied),
        name="turn",
    )(owners, orbitals)


def near_kernel(counts, lhs_ref, *refs):
    piece_refs, out_ref, rhs = refs[:-2], refs[-2], refs[-1]
    rows = piece_refs[0].shape[1]
    vector = pl.program_id(0)
    piece_refs = iter(piece_refs)
    for k, pieces in enumerate(counts):
        at, start = pl.ds(k * rows, rows), 0
        for size in pieces:
            piece = next(piece_refs)

            @pl.when((vector >= start) & (vector < start + size))
            def _():
                rhs[at, :] = piece[0]

            start += size
    out_ref[0] = jnp.dot(lhs_ref[...], rhs[...], preferred_element_type=jnp.float32)


def near_sum(lhs, blocks):
    counts = [[piece.shape[0] for piece in pieces] for pieces in blocks]
    count, (_, rows, columns) = sum(counts[0]), blocks[0][0].shape
    occupied, depth = lhs.shape
    specs = [pl.BlockSpec((occupied, depth), lambda g: (0, 0))]
    for pieces in counts:
        start = 0
        for size in pieces:
            at = functools.partial(lambda start, size, g: (jnp.clip(g - start, 0, size - 1), 0, 0), start, size)
            specs.append(pl.BlockSpec((1, rows, columns), at))
            start += size
    return pl.pallas_call(
        functools.partial(near_kernel, counts),
        out_shape=jax.ShapeDtypeStruct((count, occupied, columns), jnp.float32),
        grid=(count,),
        in_specs=specs,
        out_specs=pl.BlockSpec((1, occupied, columns), lambda g: (g, 0, 0)),
        scratch_shapes=[pltpu.VMEM((depth, columns), jnp.bfloat16)],
        compiler_params=params(24),
        cost_estimate=cost(2 * count * occupied * depth * columns, 4 * count * occupied * columns),
        name="near",
    )(lhs, *(piece for pieces in blocks for piece in pieces))


def far_kernel(first, blocks, lhs_ref, near_ref, *refs):
    block_refs, (out_ref, rhs, held, sems) = refs[:blocks], refs[-4:]
    size, rows, _ = block_refs[0].shape
    tiles = sems.shape[1]
    tile = held.shape[1] // tiles
    copies = []
    for v in range(size):
        for k, block in enumerate(block_refs):
            rhs[v, k * rows : (k + 1) * rows, :] = block[v]
        for t in range(tiles):
            part = pl.ds(t * tile, tile)
            total = near_ref[first + v, part, :] + jnp.dot(
                lhs_ref[part, :], rhs[v], preferred_element_type=jnp.float32
            )
            held[v, part, :] = total.astype(held.dtype)
            copy = pltpu.make_async_copy(
                held.at[v, part, :], out_ref.at[first + v, part, :], sems.at[v, t]
            )
            copy.start()
            copies.append(copy)
    for copy in copies:
        copy.wait()


def far_sum(lhs, near, blocks, rotated, first):
    size, _, columns = blocks[0].shape
    occupied, depth = lhs.shape
    tiles = 4
    given = [] if rotated is None else [rotated]
    whole, left = pl.BlockSpec(memory_space=pltpu.VMEM), pl.BlockSpec(memory_space=pl.ANY)
    return pl.pallas_call(
        functools.partial(far_kernel, first, len(blocks)),
        out_shape=jax.ShapeDtypeStruct(near.shape, jnp.bfloat16),
        in_specs=[whole] * (2 + len(blocks)) + [left] * len(given),
        out_specs=left,
        scratch_shapes=[
            pltpu.VMEM((size, depth, columns), jnp.bfloat16),
            pltpu.VMEM((size, occupied, columns), jnp.bfloat16),
            pltpu.SemaphoreType.DMA((size, tiles)),
        ],
        input_output_aliases={2 + len(blocks): 0} if given else {},
        compiler_params=params(20),
        cost_estimate=cost(2 * size * occupied * depth * columns, 4 * size * occupied * columns),
        name="far",
    )(lhs, near, *blocks, *given)


def middle_kernel(vector, lhs_ref, near_ref, *refs):
    block_refs, out_ref = refs[:-1], refs[-1]
    rows = block_refs[0].shape[1]
    tile = out_ref.shape[0] // 4
    for t in range(4):
        at = pl.ds(t * tile, tile)
        total = near_ref[vector, at, :]
        for k, block in enumerate(block_refs):
            total += jnp.dot(
                lhs_ref[at, k * rows : (k + 1) * rows], block[0], preferred_element_type=jnp.float32
            )
        out_ref[at, :] = total


def middle_sum(lhs, near, blocks, vector):
    _, rows, columns = blocks[0].shape
    occupied = lhs.shape[0]
    return pl.pallas_call(
        functools.partial(middle_kernel, vector),
        out_shape=jax.ShapeDtypeStruct((occupied, columns), jnp.float32),
        in_specs=[pl.BlockSpec(memory_space=pltpu.VMEM)] * (2 + len(blocks)),
        out_specs=pl.BlockSpec(memory_space=pltpu.VMEM),
        compiler_params=params(16),
        cost_estimate=cost(2 * occupied * rows * columns * len(blocks), 8 * occupied * columns),
        name="middle",
    )(lhs, near, *blocks)


def last_kernel(vector, start, lhs_ref, near_ref, block_ref, _, out_ref, held, sems):
    _, rows, columns = block_ref.shape
    at_columns, weights = pl.ds(start, columns), pl.ds(lhs_ref.shape[1] - rows, rows)
    tiles = sems.shape[0]
    tile = held.shape[0] // tiles
    copies = []
    for t in range(tiles):
        at = pl.ds(t * tile, tile)
        total = near_ref[at, at_columns] + jnp.dot(
            lhs_ref[at, weights], block_ref[0], preferred_element_type=jnp.float32
        )
        held[at, :] = total.astype(held.dtype)
        copies.append(
            pltpu.make_async_copy(held.at[at, :], out_ref.at[vector, at, at_columns], sems.at[t])
        )
        copies[-1].start()
    for copy in copies:
        copy.wait()


def last_sum(lhs, near, block, rotated, vector, start):
    _, rows, columns = block.shape
    occupied, tiles = lhs.shape[0], 8
    whole, left = pl.BlockSpec(memory_space=pltpu.VMEM), pl.BlockSpec(memory_space=pl.ANY)
    return pl.pallas_call(
        functools.partial(last_kernel, vector, start),
        out_shape=jax.ShapeDtypeStruct(rotated.shape, rotated.dtype),
        in_specs=[whole, whole, whole, left],
        out_specs=left,
        scratch_shapes=[
            pltpu.VMEM((occupied, columns), rotated.dtype),
            pltpu.SemaphoreType.DMA((tiles,)),
        ],
        input_output_aliases={3: 0},
        compiler_params=pltpu.CompilerParams(vmem_limit_bytes=16 * MIB),
        cost_estimate=cost(2 * occupied * rows * columns, 4 * occupied * columns),
        name="last",
    )(lhs, near, block, rotated)


def local(owners, chol, orbitals, greens, shift):
    walkers = greens.shape[2] // chol.shape[2]
    count = chol.shape[0] // owners
    rows, columns = chol.shape[1:]
    me, mine = lax.axis_index("orb"), lax.axis_index("walk")
    first, second, far_offsets = offsets(owners)

    def swap(value, axis, k, size):
        return lax.ppermute(value, axis, [(i, i ^ k) for i in range(size)])

    def part(source, k, start=0, stop=count):
        return lax.dynamic_slice_in_dim(source, (me ^ k) * count + start, stop - start, 0)

    source, near = chol, {k: [] for k in first}
    for start, stop in ((0, 1), (1, count)):
        if start == 0:
            pieces = first_pieces(chol, first, count, stop)
        else:
            pieces = [part(source, k, start, stop) for k in first]
        source, orbitals, greens = tied((source, orbitals, greens), *pieces)
        for k, piece in zip(first, pieces):
            near[k].append(swap(piece, "orb", k, owners))

    orbitals, greens = tied((orbitals, greens), *(near[k][0] for k in first))
    orbital_rows = lax.dynamic_slice_in_dim(orbitals, me * rows, rows, 0)
    products = jnp.dot(orbital_rows, greens[0], preferred_element_type=jnp.float32)
    products = products.astype(jnp.bfloat16)
    pieces = [
        lax.dynamic_slice_in_dim(products, (mine ^ k) * columns, columns, 1) for k in range(walkers)
    ]
    source = tied(source, *pieces)
    arrived = pieces[:1] + [swap(pieces[k], "walk", k, walkers) for k in range(1, walkers)]

    pieces = {k: part(source, k) for k in [0] + second}
    source = tied(source, *pieces.values())
    near[0] = [pieces[0]]
    for k in second:
        near[k] = [swap(pieces[k], "orb", k, owners)]

    cuts = [(a, b) for a, b in ((0, count - 2), (count - 2, count - 1)) if a < b]
    pieces = [part(source, k, *cuts[0]) for k in far_offsets]
    far = [[swap(piece, "orb", k, owners) for k, piece in zip(far_offsets, pieces)]]

    order = [0] + first + second
    lhs_near = turned(orbitals, jnp.array(order, jnp.int32) ^ me, rows)
    lhs_far = turned(orbitals, jnp.array(far_offsets, jnp.int32) ^ me, rows)

    terms = force_terms(chol, arrived, jnp.stack([me, mine]).astype(jnp.int32), count)
    terms = terms.sum(axis=(2, 3))
    total = terms[0] + sum(swap(terms[k], "walk", k, walkers) for k in range(1, walkers))
    total = total.reshape(owners, count)
    even = total[0::2] + swap(total[1::2], "orb", 1, owners)
    sums = [swap(even[k : k + 1], "orb", 2 * k, owners) for k in range(1, owners // 2)]

    source = tied(source, even)
    for n, span in enumerate(cuts[1:], 1):
        pieces = [part(source, k, *span) for k in far_offsets]
        far.append([swap(piece, "orb", k, owners) for k, piece in zip(far_offsets, pieces)])
    pieces = [part(source, k, count - 1) for k in far_offsets]
    middle = [swap(piece, "orb", k, owners) for k, piece in zip(far_offsets[:-1], pieces)]
    half = columns // last_parts(columns)
    last = [
        swap(pieces[-1][..., at : at + half], "orb", far_offsets[-1], owners)
        for at in range(0, columns, half)
    ]

    partial = near_sum(lhs_near, [near[k] for k in order])
    sums = tied(sums, partial)
    force_bias = even[:1] + sum(sums) - shift[None, :]
    rotated = None
    for (start, _), blocks in zip(cuts, far):
        rotated = far_sum(lhs_far, partial, blocks, rotated, start)
    partial = middle_sum(lhs_far, partial, middle, count - 1)
    for n, block in enumerate(last):
        rotated = last_sum(lhs_far, partial, block, rotated, count - 1, n * half)
    return force_bias, rotated


def solution(mesh):
    in_specs = (P(None, "orb", "walk"), P(), P("walk", None, None), P("orb"))
    out_specs = (P("walk", "orb"), P("orb", None, "walk"))
    owners = mesh.shape["orb"]

    def step(chol, *args):
        def body(*args):
            return local(owners, *args)

        run = jax.shard_map(
            body, mesh=mesh, in_specs=in_specs, out_specs=out_specs, check_vma=False
        )
        return run(chol, *args)

    return step
```

```python
import functools

import jax
import jax.numpy as jnp
from jax import lax
from jax.experimental import pallas as pl
from jax.experimental.pallas import tpu as pltpu
from jax.sharding import PartitionSpec as P


MIB = 2**20


def tied(value, *after):
    return lax.optimization_barrier((value, *after))[0]


def params(mib):
    return pltpu.CompilerParams(vmem_limit_bytes=mib * MIB)


def offsets(owners):
    chips = lambda k: (k >> 1).bit_count()
    first = [k for k in range(owners - 2, 0, -2) if chips(k) == 1]
    second = [k + 1 for k in first] + [1]
    return first, second, [k for k in range(1, owners) if chips(k) > 1]


def last_parts():
    return 1


def cost(flops, moved):
    return pl.CostEstimate(flops=flops, bytes_accessed=moved, transcendentals=0)


def first_kernel(offsets, count, chol_ref, *refs):
    out_refs, sems = refs[:-1], refs[-1]
    me = lax.axis_index("orb")
    copies = []
    for n, (k, out_ref) in enumerate(zip(offsets, out_refs)):
        piece = chol_ref.at[pl.ds((me ^ k) * count, out_ref.shape[0])]
        copies.append(pltpu.make_async_copy(piece, out_ref, sems.at[n]))
        copies[-1].start()
    for copy in copies:
        copy.wait()


def first_pieces(chol, offsets, count, size):
    shape = jax.ShapeDtypeStruct((size,) + chol.shape[1:], chol.dtype)
    return pl.pallas_call(
        functools.partial(first_kernel, offsets, count),
        out_shape=[shape] * len(offsets),
        in_specs=[pl.BlockSpec(memory_space=pl.ANY)],
        out_specs=[pl.BlockSpec(memory_space=pltpu.VMEM)] * len(offsets),
        scratch_shapes=[pltpu.SemaphoreType.DMA((len(offsets),))],
        compiler_params=params(8),
        cost_estimate=cost(2**20, 4 * len(offsets) * size * chol[0].size),
        name="first",
    )(pltpu.with_memory_space_constraint(chol, pltpu.HBM))


def terms_kernel(place, chol_ref, *refs):
    product_refs, out_ref = refs[:-1], refs[-1]
    for v in range(chol_ref.shape[0]):
        block = chol_ref[v].astype(jnp.float32)
        for w, product in enumerate(product_refs):
            terms = jnp.sum(product[...].astype(jnp.float32) * block, axis=0, keepdims=True)
            out_ref[w, v] = terms


def force_terms(chol, products, me, count):
    vectors, rows, columns = chol.shape
    walkers = len(products)
    whole = pl.BlockSpec((rows, columns), lambda v, place: (0, 0))
    return pl.pallas_call(
        terms_kernel,
        out_shape=jax.ShapeDtypeStruct((walkers, vectors, 1, columns), jnp.float32),
        grid_spec=pltpu.PrefetchScalarGridSpec(
            num_scalar_prefetch=1,
            grid=(vectors // count,),
            in_specs=[pl.BlockSpec((count, rows, columns), lambda v, place: (place[0] ^ v, 0, 0))]
            + [whole] * walkers,
            out_specs=pl.BlockSpec((walkers, count, 1, columns), lambda v, place: (0, v, 0, 0)),
        ),
        compiler_params=params(12),
        cost_estimate=cost(2 * walkers * chol.size, 2 * chol.size),
        name="terms",
    )(me, pltpu.with_memory_space_constraint(chol, pltpu.HBM), *products)


def turn_kernel(place, source_ref, out_ref):
    out_ref[...] = source_ref[...].T


def turned(orbitals, owners, rows):
    occupied = orbitals.shape[1]
    blocks = owners.shape[0]
    return pl.pallas_call(
        turn_kernel,
        out_shape=jax.ShapeDtypeStruct((occupied, blocks * rows), orbitals.dtype),
        grid_spec=pltpu.PrefetchScalarGridSpec(
            num_scalar_prefetch=1,
            grid=(blocks,),
            in_specs=[pl.BlockSpec((rows, occupied), lambda k, place: (place[k], 0))],
            out_specs=pl.BlockSpec((occupied, rows), lambda k, place: (0, k)),
        ),
        compiler_params=params(8),
        cost_estimate=cost(blocks * rows * occupied * 300, 4 * blocks * rows * occupied),
        name="turn",
    )(owners, orbitals)


def near_kernel(counts, lhs_ref, *refs):
    piece_refs, out_ref, rhs = refs[:-2], refs[-2], refs[-1]
    rows = piece_refs[0].shape[1]
    vector = pl.program_id(0)
    piece_refs = iter(piece_refs)
    for k, pieces in enumerate(counts):
        at, start = pl.ds(k * rows, rows), 0
        for size in pieces:
            piece = next(piece_refs)

            @pl.when((vector >= start) & (vector < start + size))
            def _():
                rhs[at, :] = piece[0]

            start += size
    out_ref[0] = jnp.dot(lhs_ref[...], rhs[...], preferred_element_type=jnp.float32)


def near_sum(lhs, blocks):
    counts = [[piece.shape[0] for piece in pieces] for pieces in blocks]
    count, (_, rows, columns) = sum(counts[0]), blocks[0][0].shape
    occupied, depth = lhs.shape
    specs = [pl.BlockSpec((occupied, depth), lambda g: (0, 0))]
    for pieces in counts:
        start = 0
        for size in pieces:
            at = functools.partial(lambda start, size, g: (jnp.clip(g - start, 0, size - 1), 0, 0), start, size)
            specs.append(pl.BlockSpec((1, rows, columns), at))
            start += size
    return pl.pallas_call(
        functools.partial(near_kernel, counts),
        out_shape=jax.ShapeDtypeStruct((count, occupied, columns), jnp.float32),
        grid=(count,),
        in_specs=specs,
        out_specs=pl.BlockSpec((1, occupied, columns), lambda g: (g, 0, 0)),
        scratch_shapes=[pltpu.VMEM((depth, columns), jnp.bfloat16)],
        compiler_params=params(24),
        cost_estimate=cost(2 * count * occupied * depth * columns, 4 * count * occupied * columns),
        name="near",
    )(lhs, *(piece for pieces in blocks for piece in pieces))


def far_kernel(first, blocks, lhs_ref, near_ref, *refs):
    block_refs, (out_ref, rhs, held, sems) = refs[:blocks], refs[-4:]
    size, rows, _ = block_refs[0].shape
    tiles = sems.shape[1]
    tile = held.shape[1] // tiles
    copies = []
    for v in range(size):
        for k, block in enumerate(block_refs):
            rhs[v, k * rows : (k + 1) * rows, :] = block[v]
        for t in range(tiles):
            part = pl.ds(t * tile, tile)
            total = near_ref[first + v, part, :] + jnp.dot(
                lhs_ref[part, :], rhs[v], preferred_element_type=jnp.float32
            )
            held[v, part, :] = total.astype(held.dtype)
            copy = pltpu.make_async_copy(
                held.at[v, part, :], out_ref.at[first + v, part, :], sems.at[v, t]
            )
            copy.start()
            copies.append(copy)
    for copy in copies:
        copy.wait()


def far_sum(lhs, near, blocks, rotated, first):
    size, _, columns = blocks[0].shape
    occupied, depth = lhs.shape
    tiles = 4
    given = [] if rotated is None else [rotated]
    whole, left = pl.BlockSpec(memory_space=pltpu.VMEM), pl.BlockSpec(memory_space=pl.ANY)
    return pl.pallas_call(
        functools.partial(far_kernel, first, len(blocks)),
        out_shape=jax.ShapeDtypeStruct(near.shape, jnp.bfloat16),
        in_specs=[whole] * (2 + len(blocks)) + [left] * len(given),
        out_specs=left,
        scratch_shapes=[
            pltpu.VMEM((size, depth, columns), jnp.bfloat16),
            pltpu.VMEM((size, occupied, columns), jnp.bfloat16),
            pltpu.SemaphoreType.DMA((size, tiles)),
        ],
        input_output_aliases={2 + len(blocks): 0} if given else {},
        compiler_params=params(20),
        cost_estimate=cost(2 * size * occupied * depth * columns, 4 * size * occupied * columns),
        name="far",
    )(lhs, near, *blocks, *given)


def middle_kernel(vector, lhs_ref, near_ref, *refs):
    block_refs, out_ref = refs[:-1], refs[-1]
    rows = block_refs[0].shape[1]
    tile = out_ref.shape[0] // 4
    for t in range(4):
        at = pl.ds(t * tile, tile)
        total = near_ref[vector, at, :]
        for k, block in enumerate(block_refs):
            total += jnp.dot(
                lhs_ref[at, k * rows : (k + 1) * rows], block[0], preferred_element_type=jnp.float32
            )
        out_ref[at, :] = total


def middle_sum(lhs, near, blocks, vector):
    _, rows, columns = blocks[0].shape
    occupied = lhs.shape[0]
    return pl.pallas_call(
        functools.partial(middle_kernel, vector),
        out_shape=jax.ShapeDtypeStruct((occupied, columns), jnp.float32),
        in_specs=[pl.BlockSpec(memory_space=pltpu.VMEM)] * (2 + len(blocks)),
        out_specs=pl.BlockSpec(memory_space=pltpu.VMEM),
        compiler_params=params(16),
        cost_estimate=cost(2 * occupied * rows * columns * len(blocks), 8 * occupied * columns),
        name="middle",
    )(lhs, near, *blocks)


def last_kernel(vector, start, lhs_ref, near_ref, block_ref, _, out_ref, held, sems):
    _, rows, columns = block_ref.shape
    at_columns, weights = pl.ds(start, columns), pl.ds(lhs_ref.shape[1] - rows, rows)
    tiles = sems.shape[0]
    tile = held.shape[0] // tiles
    copies = []
    for t in range(tiles):
        at = pl.ds(t * tile, tile)
        total = near_ref[at, at_columns] + jnp.dot(
            lhs_ref[at, weights], block_ref[0], preferred_element_type=jnp.float32
        )
        held[at, :] = total.astype(held.dtype)
        copies.append(
            pltpu.make_async_copy(held.at[at, :], out_ref.at[vector, at, at_columns], sems.at[t])
        )
        copies[-1].start()
    for copy in copies:
        copy.wait()


def last_sum(lhs, near, block, rotated, vector, start):
    _, rows, columns = block.shape
    occupied, tiles = lhs.shape[0], 8
    whole, left = pl.BlockSpec(memory_space=pltpu.VMEM), pl.BlockSpec(memory_space=pl.ANY)
    return pl.pallas_call(
        functools.partial(last_kernel, vector, start),
        out_shape=jax.ShapeDtypeStruct(rotated.shape, rotated.dtype),
        in_specs=[whole, whole, whole, left],
        out_specs=left,
        scratch_shapes=[
            pltpu.VMEM((occupied, columns), rotated.dtype),
            pltpu.SemaphoreType.DMA((tiles,)),
        ],
        input_output_aliases={3: 0},
        compiler_params=params(16),
        cost_estimate=cost(2 * occupied * rows * columns, 4 * occupied * columns),
        name="last",
    )(lhs, near, block, rotated)


def local(owners, chol, orbitals, greens, shift):
    walkers = greens.shape[2] // chol.shape[2]
    count = chol.shape[0] // owners
    rows, columns = chol.shape[1:]
    me, mine = lax.axis_index("orb"), lax.axis_index("walk")
    first, second, far_offsets = offsets(owners)

    def swap(value, axis, k, size):
        return lax.ppermute(value, axis, [(i, i ^ k) for i in range(size)])

    def part(source, k, start=0, stop=count):
        return lax.dynamic_slice_in_dim(source, (me ^ k) * count + start, stop - start, 0)

    source, near = chol, {k: [] for k in first}
    for start, stop in ((0, 1), (1, count)):
        if start == 0:
            pieces = first_pieces(chol, first, count, stop)
        else:
            pieces = [part(source, k, start, stop) for k in first]
        source, orbitals, greens = tied((source, orbitals, greens), *pieces)
        for k, piece in zip(first, pieces):
            near[k].append(swap(piece, "orb", k, owners))

    orbitals, greens = tied((orbitals, greens), *(near[k][0] for k in first))
    orbital_rows = lax.dynamic_slice_in_dim(orbitals, me * rows, rows, 0)
    products = jnp.dot(orbital_rows, greens[0], preferred_element_type=jnp.float32)
    products = products.astype(jnp.bfloat16)
    pieces = [
        lax.dynamic_slice_in_dim(products, (mine ^ k) * columns, columns, 1) for k in range(walkers)
    ]
    source = tied(source, *pieces)
    arrived = pieces[:1] + [swap(pieces[k], "walk", k, walkers) for k in range(1, walkers)]

    pieces = {k: part(source, k) for k in [0] + second}
    source = tied(source, *pieces.values())
    near[0] = [pieces[0]]
    for k in second:
        near[k] = [swap(pieces[k], "orb", k, owners)]

    cuts = [(a, b) for a, b in ((0, count - 2), (count - 2, count - 1)) if a < b]
    pieces = [part(source, k, *cuts[0]) for k in far_offsets]
    far = [[swap(piece, "orb", k, owners) for k, piece in zip(far_offsets, pieces)]]

    order = [0] + first + second
    lhs_near = turned(orbitals, jnp.array(order, jnp.int32) ^ me, rows)
    lhs_far = turned(orbitals, jnp.array(far_offsets, jnp.int32) ^ me, rows)

    terms = force_terms(chol, arrived, jnp.stack([me, mine]).astype(jnp.int32), count)
    terms = terms.sum(axis=(2, 3))
    total = terms[0] + sum(swap(terms[k], "walk", k, walkers) for k in range(1, walkers))
    total = total.reshape(owners, count)
    even = total[0::2] + swap(total[1::2], "orb", 1, owners)
    sums = [swap(even[k : k + 1], "orb", 2 * k, owners) for k in range(1, owners // 2)]

    source = tied(source, even)
    for n, span in enumerate(cuts[1:], 1):
        pieces = [part(source, k, *span) for k in far_offsets]
        far.append([swap(piece, "orb", k, owners) for k, piece in zip(far_offsets, pieces)])
    pieces = [part(source, k, count - 1) for k in far_offsets]
    middle = [swap(piece, "orb", k, owners) for k, piece in zip(far_offsets[:-1], pieces)]
    half = columns // last_parts()
    last = [
        swap(pieces[-1][..., at : at + half], "orb", far_offsets[-1], owners)
        for at in range(0, columns, half)
    ]

    partial = near_sum(lhs_near, [near[k] for k in order])
    sums = tied(sums, partial)
    force_bias = even[:1] + sum(sums) - shift[None, :]
    rotated = None
    for (start, _), blocks in zip(cuts, far):
        rotated = far_sum(lhs_far, partial, blocks, rotated, start)
    partial = middle_sum(lhs_far, partial, middle, count - 1)
    for n, block in enumerate(last):
        rotated = last_sum(lhs_far, partial, block, rotated, count - 1, n * half)
    return force_bias, rotated


def solution(mesh):
    in_specs = (P(None, "orb", "walk"), P(), P("walk", None, None), P("orb"))
    out_specs = (P("walk", "orb"), P("orb", None, "walk"))
    owners = mesh.shape["orb"]

    def step(chol, *args):
        def body(*args):
            return local(owners, *args)

        run = jax.shard_map(
            body, mesh=mesh, in_specs=in_specs, out_specs=out_specs, check_vma=False
        )
        return run(chol, *args)

    return step
```
